32 devices in a mesh: blk: 16 (over z, x, core), grp: 2 (over y).
Axes of the slice: x: 2, y: 2, z: 4, core: 2. Of those that a mesh axis runs over, the one named last changes fastest.
Arguments:
- orbitals: float32 [32, 110592], P(('blk', 'grp')), may hold values from -6 to 6
- occupation: float32 [32], P(('blk', 'grp')), may hold values from 0.2 to 2
Outputs:
- exchange: float32 [32, 110592], P(('blk', 'grp'))
- energy: float32 [], replicated
The draws below stay inside these ranges and needn't reach their ends.
All inputs are finite; a program needn't handle non-finite values.
Results may differ from the reference program's by a relative error of at most 0.00012.
Values sent between devices are 32-bit elements; how exact they have to be, the bound alone decides.
No kernel may reach another device: no remote copies, remote signals or barrier semaphores. Data moves between devices by JAX's collectives and lax.ppermute only.
A program may use at most 64 MiB of HBM per device.

```python
import math
import jax
import jax.numpy as jnp
from jax import lax

GRID = 48
CELLS = 110592
BLK_ORB = 2
NORB = 32
N_BLK = 16


def steps_of(own_key, shape, pieces, least, high):
    level, own = 1.0, jax.random.fold_in(own_key, 6)
    for axis_at, shards_of in pieces:
        draws = jnp.exp(jax.random.uniform(jax.random.fold_in(own, axis_at), (shards_of,), jnp.float32, least / len(pieces), high / len(pieces)))
        level = level * jnp.repeat(draws, shape[axis_at] // shards_of).reshape([-1 if axis == axis_at else 1 for axis in range(len(shape))])
    return level


def noise(stream_key, shape, width, most, cuts=(), kind=jnp.bfloat16):
    values = jax.random.normal(stream_key, shape, jnp.float32) * width
    if len(cuts) > 0:
        values = steps_of(stream_key, shape, cuts, -0.22, 0.18) * values
    return jnp.clip(values, min=-most, max=most).astype(kind)


def setup_inputs(seed: int = 0) -> dict:
    splits = jax.random.split(jax.random.key(seed), 3)
    return {
        "orbitals": noise(splits[0], (NORB, CELLS), 1.0, 6.0, ((0, 32),), jnp.float32),
        "occupation": jnp.clip(jnp.exp(math.log(2.0) - 2.3025851 * jax.random.uniform(splits[1], (NORB,), jnp.float32) ** steps_of(splits[1], (NORB,), ((0, 32),), -0.2, 0.2)), 0.2, 2.0),
    }


mixing = 0.25
screening = 0.1


def kernel_table(extent):
    indices = jnp.arange(extent, dtype=jnp.int32)
    folded = (indices + extent // 2) % extent - extent // 2
    squared = (folded.astype(jnp.float32) * (2.0 * math.pi / extent)) ** 2
    return 1.0 / (squared[:, None, None] + squared[None, :, None] + squared[None, None, :] + screening)


def reference(orbitals, occupation):
    kernel = kernel_table(GRID)
    blocks = orbitals.reshape(N_BLK, BLK_ORB, CELLS)
    weights = occupation.reshape(N_BLK, BLK_ORB)
    partners = jnp.concatenate([jnp.roll(blocks, 1, axis=0), jnp.roll(blocks, -1, axis=0)], axis=1)
    partner_weights = jnp.concatenate([jnp.roll(weights, 1, axis=0), jnp.roll(weights, -1, axis=0)], axis=1)

    def one_block(item):
        own, others, other_weights = item

        def one_orbital(single):
            density = (single[None, :] * others).reshape(-1, GRID, GRID, GRID)
            spectrum = jnp.fft.fftn(density, axes=(1, 2, 3)) * kernel
            potential = jnp.real(jnp.fft.ifftn(spectrum, axes=(1, 2, 3))).reshape(others.shape)
            return -mixing * jnp.sum(other_weights[:, None] * others * potential, axis=0)

        return lax.map(one_orbital, own)

    exchange = lax.map(one_block, (blocks, partners, partner_weights)).reshape(NORB, CELLS)
    energy = jnp.sum(occupation[:, None] * orbitals * exchange) / (2.0 * CELLS * NORB)
    return exchange, energy
```

```python
import math
import numpy as np
import jax
import jax.numpy as jnp
from jax import lax
from jax.sharding import PartitionSpec as P
from jax.experimental import pallas as pl
from jax.experimental.pallas import tpu as pltpu

mixing = 0.25
screening = 0.1
LANES = 128
F32 = jnp.float32


def split(values):
    values = np.asarray(values, np.float64)
    high = values.astype(jnp.bfloat16).astype(np.float64)
    low = (values - high).astype(jnp.bfloat16).astype(np.float64)
    return high.astype(np.float32), low.astype(np.float32)


def basis(extent):
    n = np.arange(extent)
    rows, freqs = [], []
    half = extent // 2
    rows += [np.full(extent, math.sqrt(1.0 / extent)), np.where(n % 2 == 0, 1.0, -1.0) * math.sqrt(1.0 / extent)]
    freqs += [0, half]
    for k in range(1, half):
        angle = 2.0 * math.pi * ((k * n) % extent) / extent
        rows += [math.sqrt(2.0 / extent) * np.cos(angle), math.sqrt(2.0 / extent) * np.sin(angle)]
        freqs += [k, k]
    return np.stack(rows), np.array(freqs)


def lane_table(matrix):
    extent = matrix.shape[0]
    high, low = split(matrix)
    table = np.zeros((2 * LANES, 2 * LANES), np.float32)
    for part in range(2):
        for pair in range(2):
            r = part * LANES + pair * extent
            c = pair * extent
            table[r:r + extent, c:c + extent] = high
            table[r:r + extent, LANES + c:LANES + c + extent] = low
    return table


def row_table(matrix):
    high, low = split(matrix)
    return np.concatenate([high, high, low], axis=1)


def low_of(x):
    return x - x.astype(jnp.bfloat16).astype(F32)


def rows_apply(table, x):
    return jnp.dot(table, jnp.concatenate([x, low_of(x), x], axis=0), preferred_element_type=F32)


def lanes_apply(x, table):
    both = jnp.dot(jnp.concatenate([x, low_of(x)], axis=1), table, preferred_element_type=F32)
    return both[:, :LANES] + both[:, LANES:]


def kernel_body(extent, w_own_ref, w_par_ref, w_prev_ref, own_ref, par_ref, prev_ref, fz_ref, iz_ref, fr_ref, ir_ref, kern_ref,
                mine_ref, topar_ref, toprev_ref, e_ref, t_ref):
    pitch = t_ref.shape[0] // extent
    tiles = 3
    per = tiles * LANES // extent
    runs = extent // per
    row_stride = tiles * runs
    lane = lax.broadcasted_iota(jnp.int32, (extent, LANES), 1)
    fr, ir = fr_ref[...], ir_ref[...]

    def dense(ref, y1, t):
        return ref[pl.ds(tiles * y1 + t, extent, stride=row_stride), :]

    def pick(parts, start):
        t, off = divmod(start, LANES)
        if off + extent <= LANES:
            return parts[t], off
        return jnp.where(lane >= off, parts[t], parts[t + 1]), off

    def turn(x, shift):
        shift %= LANES
        return x if shift == 0 else pltpu.roll(x, shift, 1)

    for y1 in range(runs):
        prev = [dense(prev_ref, y1, t) for t in range(tiles)]
        first = [dense(own_ref, y1, t) * prev[t] for t in range(tiles)]
        second = [dense(par_ref, y1, t) * prev[t] for t in range(tiles)]
        rows = []
        for y0 in range(per):
            a, off = pick(first, y0 * extent)
            b, _ = pick(second, y0 * extent)
            rows.append(jnp.where(lane < extent, turn(a, -off), turn(b, extent - off)))
        after = lanes_apply(jnp.concatenate(rows, axis=0), fz_ref[...])
        for y0 in range(0, per, 2):
            two = jnp.concatenate([after[y0 * extent:(y0 + 1) * extent], after[(y0 + 1) * extent:(y0 + 2) * extent]], axis=1)
            out = rows_apply(fr, two)
            y = y1 * per + y0
            t_ref[pl.ds(y * pitch, extent), :] = out[:, :LANES]
            t_ref[pl.ds((y + 1) * pitch, extent), :] = out[:, LANES:]

    for p in range(extent // 2):
        two = jnp.concatenate([t_ref[pl.ds(2 * p, extent, stride=pitch), :], t_ref[pl.ds(2 * p + 1, extent, stride=pitch), :]], axis=1)
        out = rows_apply(fr, two)
        if p == 0:
            k = jnp.concatenate([kern_ref[0], kern_ref[extent // 2]], axis=1)
        else:
            k = jnp.concatenate([kern_ref[p], kern_ref[p]], axis=1)
        out = rows_apply(ir, out * k)
        t_ref[pl.ds(2 * p, extent, stride=pitch), :] = out[:, :LANES]
        t_ref[pl.ds(2 * p + 1, extent, stride=pitch), :] = out[:, LANES:]

    w_own, w_par, w_prev = w_own_ref[0], w_par_ref[0], w_prev_ref[0]
    total = jnp.zeros((extent, LANES), F32)
    for y1 in range(runs):
        rows = []
        for y0 in range(0, per, 2):
            y = y1 * per + y0
            two = jnp.concatenate([t_ref[pl.ds(y * pitch, extent), :], t_ref[pl.ds((y + 1) * pitch, extent), :]], axis=1)
            out = rows_apply(ir, two)
            rows += [out[:, :LANES], out[:, LANES:]]
        after = lanes_apply(jnp.concatenate(rows, axis=0), iz_ref[...])
        pieces = [after[y0 * extent:(y0 + 1) * extent] for y0 in range(per)]
        for t in range(tiles):
            v = [None, None]
            for y0 in range(per):
                start = y0 * extent - t * LANES
                if start >= LANES or start + extent <= 0:
                    continue
                for pair in range(2):
                    moved = turn(pieces[y0], start - pair * extent)
                    v[pair] = moved if v[pair] is None else jnp.where(lane >= start, moved, v[pair])
            prev, own, par = dense(prev_ref, y1, t), dense(own_ref, y1, t), dense(par_ref, y1, t)
            rows_at = pl.ds(tiles * y1 + t, extent, stride=row_stride)
            one, two = w_prev * (prev * v[0]), w_prev * (prev * v[1])
            mine_ref[rows_at, :] = one
            topar_ref[rows_at, :] = two
            toprev_ref[rows_at, :] = (w_own * own) * v[0] + (w_par * par) * v[1]
            total = total + ((w_own * own) * one + (w_par * par) * two)
    e_ref[...] = jnp.full(e_ref.shape, jnp.sum(total), F32)


def pair_call(weights, own, par, prev, count):
    cells = own.size
    extent = round(cells ** (1.0 / 3.0))
    matrix, freqs = basis(extent)
    ksq = (2.0 * math.pi / extent * freqs) ** 2
    kzl = np.zeros(LANES)
    kzl[:extent] = ksq
    kzl[extent:2 * extent] = ksq
    distinct = (2.0 * math.pi / extent * np.arange(extent // 2 + 1)) ** 2
    kern = (1.0 / (distinct[:, None, None] + ksq[None, :, None] + kzl[None, None, :] + screening)).astype(np.float32)
    pitch = extent + 8
    dense = jax.ShapeDtypeStruct((cells // LANES, LANES), F32)
    shape = lambda a: a.reshape(cells // LANES, LANES)
    vm = pl.BlockSpec(memory_space=pltpu.VMEM)
    return pl.pallas_call(
        lambda *refs: kernel_body(extent, *refs),
        out_shape=(dense, dense, dense, jax.ShapeDtypeStruct((count, LANES), F32)),
        in_specs=[pl.BlockSpec(memory_space=pltpu.SMEM)] * 3 + [vm] * 8,
        out_specs=(vm, vm, vm, vm),
        scratch_shapes=[pltpu.VMEM((extent * pitch, LANES), F32)],
        name="pairs",
    )(*weights, shape(own), shape(par), shape(prev), jnp.asarray(lane_table(matrix.T)), jnp.asarray(lane_table(matrix)),
      jnp.asarray(row_table(matrix)), jnp.asarray(row_table(matrix.T)), jnp.asarray(kern))


AXES = ("blk", "grp")


def moved(value, blocks, groups):
    n_blk, n_grp = lax.axis_size("blk"), lax.axis_size("grp")
    pairs = [(b * n_grp + g, (b + blocks) % n_blk * n_grp + (g + groups) % n_grp)
             for b in range(n_blk) for g in range(n_grp)]
    return lax.ppermute(value, AXES, pairs)


def local(orbitals, occupation):
    count = lax.axis_size(AXES)
    cells = orbitals.shape[1]
    partner, w_partner = moved(orbitals, 0, 1), moved(occupation, 0, 1)
    previous, w_previous = moved(orbitals, 1, 0), moved(occupation, 1, 0)
    mine, to_partner, to_previous, shares = pair_call(
        (occupation, w_partner, w_previous), orbitals, partner, previous, count)
    back = moved(to_partner, 0, 1)
    behind = moved(to_previous, -1, 0)
    everyone = lax.all_to_all(shares, AXES, 0, 0, tiled=True)
    exchange = (-mixing * (mine + back + behind)).reshape(1, cells)
    energy = jnp.sum(everyone[:, 0]) * (-2.0 * mixing / (2.0 * cells * orbitals.shape[0] * count))
    return exchange, energy


def solution(mesh):
    return jax.shard_map(local, mesh=mesh, in_specs=(P(AXES, None), P(AXES)),
                         out_specs=(P(AXES, None), P()), check_vma=False)
```

```python
import math
import numpy as np
import jax
import jax.numpy as jnp
from jax import lax
from jax.sharding import PartitionSpec as P
from jax.experimental import pallas as pl
from jax.experimental.pallas import tpu as pltpu

mixing = 0.25
screening = 0.1
LANES = 128
F32 = jnp.float32
PAD = 8
LIMIT = 12 * 1024 * 1024


def split(values):
    values = np.asarray(values, np.float64)
    high = values.astype(jnp.bfloat16).astype(np.float64)
    low = (values - high).astype(jnp.bfloat16).astype(np.float64)
    return high.astype(np.float32), low.astype(np.float32)


def basis(extent):
    n, half = np.arange(extent), extent // 2
    rows = [np.full(extent, math.sqrt(1.0 / extent)), (1.0 - 2.0 * (n % 2)) * math.sqrt(1.0 / extent)]
    freqs = [0, half]
    for k in range(1, half):
        angle = 2.0 * math.pi * ((k * n) % extent) / extent
        rows += [math.sqrt(2.0 / extent) * np.cos(angle), math.sqrt(2.0 / extent) * np.sin(angle)]
        freqs += [k, k]
    return np.stack(rows), np.array(freqs)


def odd_basis(extent):
    n, rows, freqs = np.arange(extent), [], []
    for k in range(1, extent, 2):
        angle = math.pi * ((k * n) % (2 * extent)) / extent
        rows += [math.sqrt(2.0 / extent) * np.cos(angle), math.sqrt(2.0 / extent) * np.sin(angle)]
        freqs += [k, k]
    return np.stack(rows), np.array(freqs)


def lane_table(matrix):
    size = matrix.shape[0]
    table = np.zeros((2 * LANES, 2 * LANES), np.float32)
    for part in range(2):
        for col, values in enumerate(split(matrix)):
            table[part * LANES:part * LANES + size, col * LANES:col * LANES + size] = values
    return table


def row_table(matrix):
    high, low = split(matrix)
    return np.concatenate([high, high, low], axis=1)


def tables(extent):
    half = extent // 2
    full, freqs = basis(extent)
    even, even_freqs = basis(half)
    odd, odd_freqs = odd_basis(half)
    fold = np.array([[1.0, 1.0], [1.0, -1.0]]) / math.sqrt(2.0)
    square = lambda f: (2.0 * math.pi / extent * np.asarray(f, np.float64)) ** 2
    lanes = np.zeros((half, LANES))
    lanes[:, :extent] = square(2 * even_freqs)[:, None] + square(freqs)[None, :]
    lanes[:, extent:2 * extent] = square(odd_freqs)[:, None] + square(freqs)[None, :]
    kern = 1.0 / (square(np.arange(half + 1))[:, None, None] + lanes[None] + screening)
    return [jnp.asarray(t, F32) for t in (
        lane_table(np.kron(fold, full.T)), lane_table(np.kron(fold, full)),
        row_table(full), row_table(full.T),
        row_table(np.concatenate([even, odd])), row_table(np.concatenate([even.T, odd.T])), kern)]


def place_body(count, *refs):
    sems = refs[2 * count]
    copies = [pltpu.make_async_copy(refs[i], refs[count + i], sems.at[i]) for i in range(count)]
    for copy in copies:
        copy.start()
    for copy in copies:
        copy.wait()


def placed(*arrays):
    arrays = [pltpu.with_memory_space_constraint(a, pltpu.HBM) for a in arrays]
    return pl.pallas_call(
        lambda *refs: place_body(len(arrays), *refs),
        out_shape=[pltpu.VMEM(a.shape, F32) for a in arrays],
        in_specs=[pl.BlockSpec(memory_space=pltpu.HBM)] * len(arrays),
        out_specs=[pl.BlockSpec(memory_space=pltpu.VMEM)] * len(arrays),
        scratch_shapes=[pltpu.SemaphoreType.DMA((len(arrays),))],
        compiler_params=pltpu.CompilerParams(vmem_limit_bytes=LIMIT),
        name="place",
    )(*arrays)


def low_of(x):
    return x - x.astype(jnp.bfloat16).astype(F32)


def rows_apply(table, x):
    return jnp.dot(table, jnp.concatenate([x, low_of(x), x], axis=0), preferred_element_type=F32)


def lanes_apply(x, table):
    both = jnp.dot(jnp.concatenate([x, low_of(x)], axis=1), table, preferred_element_type=F32)
    return both[:, :LANES] + both[:, LANES:]


def beside(a, b):
    return jnp.concatenate([a, b], axis=1)


def pair_body(extent, adds, *refs):
    first_ref, prev_ref, fz_ref, iz_ref, fx_ref, ix_ref, fy_ref, iy_ref, kern_ref = refs[:9]
    if adds:
        weights_hbm, (more_ref, more_e_ref) = refs[9:12], refs[12:14]
        to_first_ref, to_prev_ref, e_ref, w_out_ref, t_ref, w_ref, sems = refs[14:]
        fetches = [pltpu.make_async_copy(weights_hbm[i], w_ref.at[i], sems.at[i]) for i in range(3)]
        for fetch in fetches:
            fetch.start()
    else:
        to_first_ref, to_prev_ref, e_ref, t_ref = refs[9:]
    half = extent // 2
    pitch = t_ref.shape[0] // half
    tiles = 3
    per = tiles * LANES // extent
    runs = extent // per
    row_stride = tiles * runs
    lane = lax.broadcasted_iota(jnp.int32, (extent, LANES), 1)
    low_half = lax.broadcasted_iota(jnp.int32, (half, 2 * LANES), 1) % LANES < extent
    fx, ix, fy, iy = fx_ref[...], ix_ref[...], fy_ref[...], iy_ref[...]

    def dense(ref, y1, t):
        return ref[pl.ds(tiles * y1 + t, extent, stride=row_stride), :]

    def pick(parts, start):
        t, off = divmod(start, LANES)
        if off + extent <= LANES:
            return parts[t], off
        return jnp.where(lane >= off, parts[t], parts[t + 1]), off

    def turn(x, shift):
        shift %= LANES
        return x if shift == 0 else pltpu.roll(x, shift, 1)

    for y1 in range(runs // 2):
        parts = [[dense(first_ref, y1 + h * (runs // 2), t) * dense(prev_ref, y1 + h * (runs // 2), t)
                  for t in range(tiles)] for h in range(2)]
        rows = []
        for y0 in range(per):
            a, off = pick(parts[0], y0 * extent)
            b, _ = pick(parts[1], y0 * extent)
            rows.append(jnp.where(lane < extent, turn(a, -off), turn(b, extent - off)))
        after = lanes_apply(jnp.concatenate(rows, axis=0), fz_ref[...])
        for y0 in range(0, per, 2):
            out = rows_apply(fx, beside(after[y0 * extent:(y0 + 1) * extent], after[(y0 + 1) * extent:(y0 + 2) * extent]))
            y = y1 * per + y0
            t_ref[pl.ds(y * pitch, extent), :] = out[:, :LANES]
            t_ref[pl.ds((y + 1) * pitch, extent), :] = out[:, LANES:]

    for p in range(half):
        at = [pl.ds(2 * p + i, half, stride=pitch) for i in range(2)]
        out = rows_apply(fy, beside(t_ref[at[0], :], t_ref[at[1], :]))
        ks = beside(kern_ref[0], kern_ref[half]) if p == 0 else beside(kern_ref[p], kern_ref[p])
        out = rows_apply(iy, jnp.where(low_half, out[:half], out[half:]) * ks)
        out = jnp.where(low_half, out[:half], out[half:])
        t_ref[at[0], :] = out[:, :LANES]
        t_ref[at[1], :] = out[:, LANES:]

    if adds:
        for fetch in fetches:
            fetch.wait()
        w_own, w_first, w_prev = (w_ref[i] for i in range(3))
    total = jnp.zeros((extent, LANES), F32)
    for y1 in range(runs // 2):
        rows = []
        for y0 in range(0, per, 2):
            y = y1 * per + y0
            out = rows_apply(ix, beside(t_ref[pl.ds(y * pitch, extent), :], t_ref[pl.ds((y + 1) * pitch, extent), :]))
            rows += [out[:, :LANES], out[:, LANES:]]
        after = lanes_apply(jnp.concatenate(rows, axis=0), iz_ref[...])
        pieces = [after[y0 * extent:(y0 + 1) * extent] for y0 in range(per)]
        for t in range(tiles):
            for h in range(2):
                v = None
                for y0 in range(per):
                    start = y0 * extent - t * LANES
                    if start < LANES and start + extent > 0:
                        piece = turn(pieces[y0], start - h * extent)
                        v = piece if v is None else jnp.where(lane >= start, piece, v)
                run = y1 + h * (runs // 2)
                prev, first = dense(prev_ref, run, t), dense(first_ref, run, t)
                at = pl.ds(tiles * run + t, extent, stride=row_stride)
                pv, fv = prev * v, first * v
                to_first_ref[at, :] = w_prev * pv if adds else pv
                to_prev_ref[at, :] = w_first * fv + w_own * more_ref[at, :] if adds else fv
                total = total + first * pv
    e_ref[...] = jnp.broadcast_to(jnp.sum(total), e_ref.shape)
    if adds:
        w_out_ref[...] = jnp.broadcast_to(w_prev, w_out_ref.shape)
        e_ref[...] = w_prev * (w_first * e_ref[...] + w_own * more_e_ref[...])


def pair_call(first, prev, constants, weights, more, count, name):
    rows = first.shape[0]
    extent = round((rows * LANES) ** (1.0 / 3.0))
    dense = jax.ShapeDtypeStruct((rows, LANES), F32)
    vm = pl.BlockSpec(memory_space=pltpu.VMEM)
    outs = [dense, dense, jax.ShapeDtypeStruct((count, LANES), F32)]
    if weights:
        outs.append(jax.ShapeDtypeStruct((1, LANES), F32))
    operands = [first, prev, *constants, *weights, *more]
    return pl.pallas_call(
        lambda *refs: pair_body(extent, 1 if more else 0, *refs),
        out_shape=outs,
        in_specs=[vm] * 9 + [pl.BlockSpec(memory_space=pl.ANY)] * len(weights) + [vm] * len(more),
        out_specs=[vm] * len(outs),
        scratch_shapes=[pltpu.VMEM((extent // 2 * (extent + PAD), LANES), F32)] + (
            [pltpu.VMEM((3, 1, 1), F32), pltpu.SemaphoreType.DMA((3,))] if weights else []),
        compiler_params=pltpu.CompilerParams(vmem_limit_bytes=LIMIT),
        name=name,
    )(*operands)


def combine_body(scale, e_scale, w_ref, mine_ref, back_ref, behind_ref, everyone_ref, out_ref, e_ref):
    out_ref[...] = scale * (w_ref[...] * mine_ref[...] + back_ref[...] + behind_ref[...])
    e_ref[...] = e_scale * jnp.sum(everyone_ref[...], axis=0, keepdims=True)[:, :1]


AXES = ("blk", "grp")


def moved(value, blocks, groups):
    n_blk, n_grp = lax.axis_size("blk"), lax.axis_size("grp")
    pairs = [(b * n_grp + g, (b + blocks) % n_blk * n_grp + (g + groups) % n_grp)
             for b in range(n_blk) for g in range(n_grp)]
    return lax.ppermute(value, AXES, pairs)


def local(orbitals, occupation):
    count = lax.axis_size(AXES)
    cells = orbitals.size
    weight = occupation.reshape(1, 1)
    own = orbitals.reshape(cells // LANES, LANES)
    previous, w_previous = moved(own, 1, 0), moved(weight, 1, 0)
    partner, w_partner = moved(own, 0, 1), moved(weight, 0, 1)
    mine_own, *constants = placed(own, *tables(round(cells ** (1.0 / 3.0))))
    mine, part, share = pair_call(mine_own, previous, constants, (), (), count, "own_pair")
    to_partner, to_previous, share, w_near = pair_call(
        partner, previous, constants, (weight, w_partner, w_previous), (part, share), count, "partner_pair")
    back = moved(to_partner, 0, 1)
    behind = moved(to_previous, -1, 0)
    everyone = lax.all_to_all(share, AXES, 0, 0, tiled=True)
    vm = pl.BlockSpec(memory_space=pltpu.VMEM)
    exchange, energy = pl.pallas_call(
        lambda *refs: combine_body(-mixing, -2.0 * mixing / (2.0 * cells * count), *refs),
        out_shape=(jax.ShapeDtypeStruct(own.shape, F32), jax.ShapeDtypeStruct((1, 1), F32)),
        in_specs=[vm] * 5, out_specs=(vm, vm),
        compiler_params=pltpu.CompilerParams(vmem_limit_bytes=LIMIT),
        name="combine",
    )(w_near, mine, back, behind, everyone)
    return exchange.reshape(orbitals.shape), energy.reshape(())


def solution(mesh):
    return jax.shard_map(local, mesh=mesh, in_specs=(P(AXES, None), P(AXES)),
                         out_specs=(P(AXES, None), P()), check_vma=False)
```

```python
import math
import numpy as np
import jax
import jax.numpy as jnp
from jax import lax
from jax.sharding import PartitionSpec as P
from jax.experimental import pallas as pl
from jax.experimental.pallas import tpu as pltpu

mixing = 0.25
screening = 0.1
LANES = 128
F32 = jnp.float32
PAD = 8
LIMIT = 12 * 1024 * 1024


def split(values):
    values = np.asarray(values, np.float64)
    high = values.astype(jnp.bfloat16).astype(np.float64)
    low = (values - high).astype(jnp.bfloat16).astype(np.float64)
    return high.astype(np.float32), low.astype(np.float32)


def basis(extent):
    n, half = np.arange(extent), extent // 2
    rows = [np.full(extent, math.sqrt(1.0 / extent)), (1.0 - 2.0 * (n % 2)) * math.sqrt(1.0 / extent)]
    freqs = [0, half]
    for k in range(1, half):
        angle = 2.0 * math.pi * ((k * n) % extent) / extent
        rows += [math.sqrt(2.0 / extent) * np.cos(angle), math.sqrt(2.0 / extent) * np.sin(angle)]
        freqs += [k, k]
    return np.stack(rows), np.array(freqs)


def odd_basis(extent):
    n, rows, freqs = np.arange(extent), [], []
    for k in range(1, extent, 2):
        angle = math.pi * ((k * n) % (2 * extent)) / extent
        rows += [math.sqrt(2.0 / extent) * np.cos(angle), math.sqrt(2.0 / extent) * np.sin(angle)]
        freqs += [k, k]
    return np.stack(rows), np.array(freqs)


def lane_table(matrix):
    size = matrix.shape[0]
    table = np.zeros((2 * LANES, 2 * LANES), np.float32)
    for part in range(2):
        for col, values in enumerate(split(matrix)):
            table[part * LANES:part * LANES + size, col * LANES:col * LANES + size] = values
    return table


def row_table(matrix):
    high, low = split(matrix)
    return np.concatenate([high, high, low], axis=1)


def tables(extent):
    half = extent // 2
    full, freqs = basis(extent)
    even, even_freqs = basis(half)
    odd, odd_freqs = odd_basis(half)
    fold = np.array([[1.0, 1.0], [1.0, -1.0]]) / math.sqrt(2.0)
    square = lambda f: (2.0 * math.pi / extent * np.asarray(f, np.float64)) ** 2
    lanes = np.zeros((half, LANES))
    lanes[:, :extent] = square(2 * even_freqs)[:, None] + square(freqs)[None, :]
    lanes[:, extent:2 * extent] = square(odd_freqs)[:, None] + square(freqs)[None, :]
    kern = 1.0 / (square(np.arange(half + 1))[:, None, None] + lanes[None] + screening)
    return [jnp.asarray(t, F32) for t in (
        lane_table(np.kron(fold, full.T)), lane_table(np.kron(fold, full)),
        row_table(full), row_table(full.T),
        row_table(np.concatenate([even, odd])), row_table(np.concatenate([even.T, odd.T])), kern)]


def place_body(count, *refs):
    sems = refs[2 * count]
    copies = [pltpu.make_async_copy(refs[i], refs[count + i], sems.at[i]) for i in range(count)]
    for copy in copies:
        copy.start()
    for copy in copies:
        copy.wait()


def placed(*arrays):
    arrays = [pltpu.with_memory_space_constraint(a, pltpu.HBM) for a in arrays]
    return pl.pallas_call(
        lambda *refs: place_body(len(arrays), *refs),
        out_shape=[pltpu.VMEM(a.shape, F32) for a in arrays],
        in_specs=[pl.BlockSpec(memory_space=pltpu.HBM)] * len(arrays),
        out_specs=[pl.BlockSpec(memory_space=pltpu.VMEM)] * len(arrays),
        scratch_shapes=[pltpu.SemaphoreType.DMA((len(arrays),))],
        compiler_params=pltpu.CompilerParams(vmem_limit_bytes=LIMIT),
        name="place",
    )(*arrays)


def low_of(x):
    return x - x.astype(jnp.bfloat16).astype(F32)


def rows_apply(table, x):
    return jnp.dot(table, jnp.concatenate([x, low_of(x), x], axis=0), preferred_element_type=F32)


def lanes_apply(x, table):
    both = jnp.dot(jnp.concatenate([x, low_of(x)], axis=1), table, preferred_element_type=F32)
    return both[:, :LANES] + both[:, LANES:]


def beside(a, b):
    return jnp.concatenate([a, b], axis=1)


def pair_body(extent, adds, *refs):
    first_ref, prev_ref, fz_ref, iz_ref, fx_ref, ix_ref, fy_ref, iy_ref, kern_ref = refs[:9]
    if adds:
        w_refs, (more_ref, more_e_ref) = refs[9:12], refs[12:14]
        to_first_ref, to_prev_ref, e_ref, t_ref = refs[14:]
    else:
        to_first_ref, to_prev_ref, e_ref, t_ref = refs[9:]
    half = extent // 2
    pitch = t_ref.shape[0] // half
    tiles = 3
    per = tiles * LANES // extent
    runs = extent // per
    row_stride = tiles * runs
    lane = lax.broadcasted_iota(jnp.int32, (extent, LANES), 1)
    low_half = lax.broadcasted_iota(jnp.int32, (half, 2 * LANES), 1) % LANES < extent
    fx, ix, fy, iy = fx_ref[...], ix_ref[...], fy_ref[...], iy_ref[...]

    def dense(ref, y1, t):
        return ref[pl.ds(tiles * y1 + t, extent, stride=row_stride), :]

    def pick(parts, start):
        t, off = divmod(start, LANES)
        if off + extent <= LANES:
            return parts[t], off
        return jnp.where(lane >= off, parts[t], parts[t + 1]), off

    def turn(x, shift):
        shift %= LANES
        return x if shift == 0 else pltpu.roll(x, shift, 1)

    for y1 in range(runs // 2):
        parts = [[dense(first_ref, y1 + h * (runs // 2), t) * dense(prev_ref, y1 + h * (runs // 2), t)
                  for t in range(tiles)] for h in range(2)]
        rows = []
        for y0 in range(per):
            a, off = pick(parts[0], y0 * extent)
            b, _ = pick(parts[1], y0 * extent)
            rows.append(jnp.where(lane < extent, turn(a, -off), turn(b, extent - off)))
        after = lanes_apply(jnp.concatenate(rows, axis=0), fz_ref[...])
        for y0 in range(0, per, 2):
            out = rows_apply(fx, beside(after[y0 * extent:(y0 + 1) * extent], after[(y0 + 1) * extent:(y0 + 2) * extent]))
            y = y1 * per + y0
            t_ref[pl.ds(y * pitch, extent), :] = out[:, :LANES]
            t_ref[pl.ds((y + 1) * pitch, extent), :] = out[:, LANES:]

    for p in range(half):
        at = [pl.ds(2 * p + i, half, stride=pitch) for i in range(2)]
        out = rows_apply(fy, beside(t_ref[at[0], :], t_ref[at[1], :]))
        ks = beside(kern_ref[0], kern_ref[half]) if p == 0 else beside(kern_ref[p], kern_ref[p])
        out = rows_apply(iy, jnp.where(low_half, out[:half], out[half:]) * ks)
        out = jnp.where(low_half, out[:half], out[half:])
        t_ref[at[0], :] = out[:, :LANES]
        t_ref[at[1], :] = out[:, LANES:]

    if adds:
        w_own, w_first, w_prev = (w_ref[:1, :] for w_ref in w_refs)
    total = jnp.zeros((extent, LANES), F32)
    for y1 in range(runs // 2):
        rows = []
        for y0 in range(0, per, 2):
            y = y1 * per + y0
            out = rows_apply(ix, beside(t_ref[pl.ds(y * pitch, extent), :], t_ref[pl.ds((y + 1) * pitch, extent), :]))
            rows += [out[:, :LANES], out[:, LANES:]]
        after = lanes_apply(jnp.concatenate(rows, axis=0), iz_ref[...])
        pieces = [after[y0 * extent:(y0 + 1) * extent] for y0 in range(per)]
        for t in range(tiles):
            for h in range(2):
                v = None
                for y0 in range(per):
                    start = y0 * extent - t * LANES
                    if start < LANES and start + extent > 0:
                        piece = turn(pieces[y0], start - h * extent)
                        v = piece if v is None else jnp.where(lane >= start, piece, v)
                run = y1 + h * (runs // 2)
                prev, first = dense(prev_ref, run, t), dense(first_ref, run, t)
                at = pl.ds(tiles * run + t, extent, stride=row_stride)
                pv, fv = prev * v, first * v
                to_first_ref[at, :] = w_prev * pv if adds else pv
                to_prev_ref[at, :] = w_first * fv + w_own * more_ref[at, :] if adds else fv
                total = total + first * pv
    e_ref[...] = jnp.broadcast_to(jnp.sum(total), e_ref.shape)
    if adds:
        e_ref[...] = w_prev * (w_first * e_ref[...] + w_own * more_e_ref[...])


def pair_call(first, prev, constants, weights, more, count, name):
    rows = first.shape[0]
    extent = round((rows * LANES) ** (1.0 / 3.0))
    dense = jax.ShapeDtypeStruct((rows, LANES), F32)
    vm = pl.BlockSpec(memory_space=pltpu.VMEM)
    outs = [dense, dense, jax.ShapeDtypeStruct((count, LANES), F32)]
    operands = [first, prev, *constants, *weights, *more]
    return pl.pallas_call(
        lambda *refs: pair_body(extent, 1 if more else 0, *refs),
        out_shape=outs,
        in_specs=[vm] * len(operands),
        out_specs=[vm] * len(outs),
        scratch_shapes=[pltpu.VMEM((extent // 2 * (extent + PAD), LANES), F32)],
        compiler_params=pltpu.CompilerParams(vmem_limit_bytes=LIMIT),
        name=name,
    )(*operands)


def combine_body(scale, e_scale, w_ref, mine_ref, back_ref, behind_ref, everyone_ref, out_ref, e_ref):
    out_ref[...] = scale * (w_ref[:1, :] * mine_ref[...] + back_ref[...] + behind_ref[...])
    e_ref[...] = e_scale * jnp.sum(everyone_ref[...], axis=0, keepdims=True)[:, :1]


AXES = ("blk", "grp")


def moved(value, blocks, groups):
    n_blk, n_grp = lax.axis_size("blk"), lax.axis_size("grp")
    pairs = [(b * n_grp + g, (b + blocks) % n_blk * n_grp + (g + groups) % n_grp)
             for b in range(n_blk) for g in range(n_grp)]
    return lax.ppermute(value, AXES, pairs)


def local(orbitals, occupation):
    count = lax.axis_size(AXES)
    cells = orbitals.size
    weight = jnp.broadcast_to(occupation[:, None], (8, LANES))
    own = orbitals.reshape(cells // LANES, LANES)
    previous, w_previous = moved(own, 1, 0), moved(weight, 1, 0)
    partner, w_partner = moved(own, 0, 1), moved(weight, 0, 1)
    mine_own, *constants = placed(own, *tables(round(cells ** (1.0 / 3.0))))
    mine, part, share = pair_call(mine_own, previous, constants, (), (), count, "own_pair")
    to_partner, to_previous, share = pair_call(
        partner, previous, constants, (weight, w_partner, w_previous), (part, share), count, "partner_pair")
    back = moved(to_partner, 0, 1)
    behind = moved(to_previous, -1, 0)
    everyone = lax.all_to_all(share, AXES, 0, 0, tiled=True)
    vm = pl.BlockSpec(memory_space=pltpu.VMEM)
    exchange, energy = pl.pallas_call(
        lambda *refs: combine_body(-mixing, -2.0 * mixing / (2.0 * cells * count), *refs),
        out_shape=(jax.ShapeDtypeStruct(own.shape, F32), jax.ShapeDtypeStruct((1, 1), F32)),
        in_specs=[vm] * 5, out_specs=(vm, vm),
        compiler_params=pltpu.CompilerParams(vmem_limit_bytes=LIMIT),
        name="combine",
    )(w_previous, mine, back, behind, everyone)
    return exchange.reshape(orbitals.shape), energy.reshape(())


def solution(mesh):
    return jax.shard_map(local, mesh=mesh, in_specs=(P(AXES, None), P(AXES)),
                         out_specs=(P(AXES, None), P()), check_vma=False)
```

```python
import math
import numpy as np
import jax
import jax.numpy as jnp
from jax import lax
from jax.sharding import PartitionSpec as P
from jax.experimental import pallas as pl
from jax.experimental.pallas import tpu as pltpu


mixing = 0.25
screening = 0.1
LANES = 128
F32 = jnp.float32
PAD = 8
LIMIT = 12 * 1024 * 1024


def split(values):
    values = np.asarray(values, np.float64)
    high = values.astype(jnp.bfloat16).astype(np.float64)
    low = (values - high).astype(jnp.bfloat16).astype(np.float64)
    return high.astype(np.float32), low.astype(np.float32)


def basis(extent):
    n, half = np.arange(extent), extent // 2
    rows = [np.full(extent, math.sqrt(1.0 / extent)), (1.0 - 2.0 * (n % 2)) * math.sqrt(1.0 / extent)]
    freqs = [0, half]
    for k in range(1, half):
        angle = 2.0 * math.pi * ((k * n) % extent) / extent
        rows += [math.sqrt(2.0 / extent) * np.cos(angle), math.sqrt(2.0 / extent) * np.sin(angle)]
        freqs += [k, k]
    return np.stack(rows), np.array(freqs)


def odd_basis(extent):
    n, rows, freqs = np.arange(extent), [], []
    for k in range(1, extent, 2):
        angle = math.pi * ((k * n) % (2 * extent)) / extent
        rows += [math.sqrt(2.0 / extent) * np.cos(angle), math.sqrt(2.0 / extent) * np.sin(angle)]
        freqs += [k, k]
    return np.stack(rows), np.array(freqs)


def lane_table(matrix):
    size = matrix.shape[0]
    table = np.zeros((2 * LANES, 2 * LANES), np.float32)
    for part in range(2):
        for col, values in enumerate(split(matrix)):
            table[part * LANES:part * LANES + size, col * LANES:col * LANES + size] = values
    return table


def row_table(matrix):
    high, low = split(matrix)
    return np.concatenate([high, high, low], axis=1)


def tables(extent):
    half = extent // 2
    full, freqs = basis(extent)
    even, even_freqs = basis(half)
    odd, odd_freqs = odd_basis(half)
    fold = np.array([[1.0, 1.0], [1.0, -1.0]]) / math.sqrt(2.0)
    square = lambda f: (2.0 * math.pi / extent * np.asarray(f, np.float64)) ** 2
    lanes = np.zeros((half, LANES))
    lanes[:, :extent] = square(2 * even_freqs)[:, None] + square(freqs)[None, :]
    lanes[:, extent:2 * extent] = square(odd_freqs)[:, None] + square(freqs)[None, :]
    kern = 1.0 / (square(np.arange(half + 1))[:, None, None] + lanes[None] + screening)
    return [jnp.asarray(t, F32) for t in (
        lane_table(np.kron(fold, full.T)), row_table(full), row_table(full.T),
        row_table(np.concatenate([even, odd])), row_table(np.concatenate([even.T, odd.T])), kern,
        lane_table(np.kron(fold, full)))]


def place_body(count, variants, *refs):
    sems = refs[2 * count]
    rolled_ref = refs[2 * count - 1]
    targets = [*refs[count:2 * count - 1], rolled_ref.at[0]]
    copies = [pltpu.make_async_copy(refs[i], targets[i], sems.at[i]) for i in range(count)]
    for copy in copies[::-1]:
        copy.start()
    copies[-1].wait()
    for i in range(1, len(variants)):
        for at in range(0, rolled_ref.shape[2], LANES):
            rolled_ref[i, :, at:at + LANES] = pltpu.roll(rolled_ref[0, :, at:at + LANES], variants[i], 1)
    for copy in copies[:-1]:
        copy.wait()


def placed(variants, *arrays):
    arrays = [pltpu.with_memory_space_constraint(a, pltpu.HBM) for a in arrays]
    shapes = [a.shape for a in arrays]
    shapes[-1] = (len(variants), *shapes[-1])
    return pl.pallas_call(
        lambda *refs: place_body(len(arrays), variants, *refs),
        out_shape=[pltpu.VMEM(s, F32) for s in shapes],
        in_specs=[pl.BlockSpec(memory_space=pltpu.HBM)] * len(arrays),
        out_specs=[pl.BlockSpec(memory_space=pltpu.VMEM)] * len(arrays),
        scratch_shapes=[pltpu.SemaphoreType.DMA((len(arrays),))],
        compiler_params=pltpu.CompilerParams(vmem_limit_bytes=LIMIT),
        name="place",
    )(*arrays)


def low_of(x):
    return x - x.astype(jnp.bfloat16).astype(F32)


def rows_apply(table, x):
    return jnp.dot(table, jnp.concatenate([x, low_of(x), x], axis=0), preferred_element_type=F32)


def lanes_apply(x, table):
    both = jnp.dot(jnp.concatenate([x, low_of(x)], axis=1), table, preferred_element_type=F32)
    return both[:, :LANES] + both[:, LANES:]


def beside(a, b):
    return jnp.concatenate([a, b], axis=1)


def pair_body(extent, adds, *refs):
    first_ref, prev_ref, fz_ref, fx_ref, ix_ref, fy_ref, iy_ref, kern_ref, iz_ref = refs[:9]
    if adds:
        w_refs, (more_ref, more_e_ref) = refs[9:12], refs[12:14]
        to_first_ref, to_prev_ref, e_ref, t_ref = refs[14:]
    else:
        to_first_ref, to_prev_ref, e_ref, t_ref = refs[9:]
    half = extent // 2
    pitch = t_ref.shape[0] // half
    tiles = math.lcm(extent, LANES) // LANES
    per = tiles * LANES // extent
    runs = extent // per
    row_stride = tiles * runs
    lane = lax.broadcasted_iota(jnp.int32, (extent, LANES), 1)
    low_half = lax.broadcasted_iota(jnp.int32, (half, 2 * LANES), 1) % LANES < extent
    fx, ix, fy, iy = fx_ref[...], ix_ref[...], fy_ref[...], iy_ref[...]

    def dense(ref, y1, t):
        return ref[pl.ds(tiles * y1 + t, extent, stride=row_stride), :]

    def row(parts, y0):
        t, off = divmod(y0 * extent, LANES)
        if off + extent <= LANES:
            a, b = parts[0][t], parts[1][t]
            inside = lane < off + extent
            if off + 2 * extent > LANES:
                inside &= lane >= off
            return jnp.where(inside, a, b)
        a = jnp.where(lane >= off, parts[0][t], parts[0][t + 1])
        b = jnp.where(lane < extent, parts[1][t], parts[1][t + 1])
        return jnp.where((lane >= off + extent - LANES) & (lane < off), b, a)

    def turned_table(off):
        if off == 0:
            return fz_ref[...]
        cuts = [fz_ref[at + s:at + e] for at in (0, LANES) for s, e in ((LANES - off, LANES), (0, LANES - off))]
        return jnp.concatenate(cuts, axis=0)

    steps = runs // 2
    parts = []
    for y1 in range(steps):
        both = [[dense(first_ref, y1 + h * steps, t) * dense(prev_ref, y1 + h * steps, t)
                 for t in range(tiles)] for h in range(2)]
        parts.append([both[0], [pltpu.roll(p, extent, 1) for p in both[1]]])

    def rows_of(y):
        return pl.ds(y * pitch, extent)

    def along_rows(table):
        for y in range(0, half, 2):
            out = rows_apply(table, beside(t_ref[rows_of(y), :], t_ref[rows_of(y + 1), :]))
            t_ref[rows_of(y), :] = out[:, :LANES]
            t_ref[rows_of(y + 1), :] = out[:, LANES:]

    for y0 in range(per):
        after = lanes_apply(jnp.concatenate([row(parts[y1], y0) for y1 in range(steps)], axis=0),
                            turned_table(y0 * extent % LANES))
        for y1 in range(steps):
            t_ref[rows_of(y1 * per + y0), :] = after[y1 * extent:(y1 + 1) * extent]
    along_rows(fx)

    for p in range(half):
        at = [pl.ds(2 * p + i, half, stride=pitch) for i in range(2)]
        out = rows_apply(fy, beside(t_ref[at[0], :], t_ref[at[1], :]))
        ks = beside(kern_ref[0], kern_ref[half]) if p == 0 else beside(kern_ref[p], kern_ref[p])
        out = rows_apply(iy, jnp.where(low_half, out[:half], out[half:]) * ks)
        out = jnp.where(low_half, out[:half], out[half:])
        t_ref[at[0], :] = out[:, :LANES]
        t_ref[at[1], :] = out[:, LANES:]

    if adds:
        w_own, w_first, w_prev = (w_ref[:1, :] for w_ref in w_refs)
    total = jnp.zeros((extent, LANES), F32)
    turned_lane = (lane + LANES - extent) % LANES
    tile_of = {}

    def finish(t):
        nonlocal total
        for y1 in range(steps):
            for h in range(2):
                v = tile_of.pop((t, y1, h))
                if h:
                    v = pltpu.roll(v, LANES - extent, 1)
                run = y1 + h * steps
                prev, first = dense(prev_ref, run, t), dense(first_ref, run, t)
                at = pl.ds(tiles * run + t, extent, stride=row_stride)
                pv, fv = prev * v, first * v
                to_first_ref[at, :] = w_prev * pv if adds else pv
                to_prev_ref[at, :] = w_first * fv + w_own * more_ref[at, :] if adds else fv
                total = total + first * pv

    along_rows(ix)
    for y0 in range(per):
        start = y0 * extent
        after = lanes_apply(jnp.concatenate([t_ref[rows_of(y1 * per + y0), :] for y1 in range(steps)], axis=0), iz_ref[y0])
        for t in range(start // LANES, (start + extent - 1) // LANES + 1):
            for y1 in range(steps):
                piece = after[y1 * extent:(y1 + 1) * extent]
                for h in range(2):
                    held = tile_of.get((t, y1, h))
                    where = turned_lane if h else lane
                    tile_of[t, y1, h] = piece if held is None else jnp.where(where >= start - t * LANES, piece, held)
        if (start + extent) // LANES > start // LANES:
            finish(start // LANES)
    e_ref[...] = jnp.broadcast_to(jnp.sum(total), e_ref.shape)
    if adds:
        e_ref[...] = w_prev * (w_first * e_ref[...] + w_own * more_e_ref[...])


def pair_call(first, prev, constants, weights, more, count):
    rows = first.shape[0]
    extent = round((rows * LANES) ** (1.0 / 3.0))
    dense = jax.ShapeDtypeStruct((rows, LANES), F32)
    vm = pl.BlockSpec(memory_space=pltpu.VMEM)
    outs = [dense, dense, jax.ShapeDtypeStruct((count, LANES), F32)]
    operands = [first, prev, *constants, *weights, *more]
    return pl.pallas_call(
        lambda *refs: pair_body(extent, 1 if more else 0, *refs),
        out_shape=outs,
        in_specs=[vm] * len(operands),
        out_specs=[vm] * len(outs),
        scratch_shapes=[pltpu.VMEM((extent // 2 * (extent + PAD), LANES), F32)],
        compiler_params=pltpu.CompilerParams(vmem_limit_bytes=LIMIT),
    )(*operands)


def combine_body(scale, e_scale, w_ref, mine_ref, back_ref, behind_ref, everyone_ref, out_ref, e_ref):
    out_ref[...] = scale * (w_ref[:1, :] * mine_ref[...] + back_ref[...] + behind_ref[...])
    e_ref[...] = e_scale * jnp.sum(everyone_ref[...], axis=0, keepdims=True)[:, :1]


AXES = ("blk", "grp")


def moved(value, blocks, groups):
    n_blk, n_grp = lax.axis_size("blk"), lax.axis_size("grp")
    pairs = [(b * n_grp + g, (b + blocks) % n_blk * n_grp + (g + groups) % n_grp)
             for b in range(n_blk) for g in range(n_grp)]
    return lax.ppermute(value, AXES, pairs)


def local(orbitals, occupation):
    count = lax.axis_size(AXES)
    cells = orbitals.size
    weight = jnp.broadcast_to(occupation[:, None], (8, LANES))
    own = orbitals.reshape(cells // LANES, LANES)
    partner = moved(own, 0, 1)
    previous = moved(own, 1, 0)
    w_partner, w_previous = moved(weight, 0, 1), moved(weight, 1, 0)
    extent = round(cells ** (1.0 / 3.0))
    variants = [y0 * extent % LANES for y0 in range(math.lcm(extent, LANES) // extent)]
    mine_own, *constants = placed(variants, own, *tables(extent))
    mine, part, share = pair_call(mine_own, previous, constants, (), (), count)
    to_partner, to_previous, share = pair_call(
        partner, previous, constants, (weight, w_partner, w_previous), (part, share), count)
    back = moved(to_partner, 0, 1)
    behind = moved(to_previous, -1, 0)
    everyone = lax.all_to_all(share, AXES, 0, 0, tiled=True)
    vm = pl.BlockSpec(memory_space=pltpu.VMEM)
    exchange, energy = pl.pallas_call(
        lambda *refs: combine_body(-mixing, -2.0 * mixing / (2.0 * cells * count), *refs),
        out_shape=(jax.ShapeDtypeStruct(own.shape, F32), jax.ShapeDtypeStruct((1, 1), F32)),
        in_specs=[vm] * 5, out_specs=(vm, vm),
        compiler_params=pltpu.CompilerParams(vmem_limit_bytes=LIMIT),
        name="combine",
    )(w_previous, mine, back, behind, everyone)
    return exchange.reshape(orbitals.shape), energy.reshape(())


def solution(mesh):
    return jax.shard_map(local, mesh=mesh, in_specs=(P(AXES, None), P(AXES)),
                         out_specs=(P(AXES, None), P()), check_vma=False)
```

```python
import math
import numpy as np
import jax
import jax.numpy as jnp
from jax import lax
from jax.sharding import PartitionSpec as P
from jax.experimental import pallas as pl
from jax.experimental.pallas import tpu as pltpu


mixing = 0.25
screening = 0.1
LANES = 128
F32 = jnp.float32
PAD = 8
PARTS = 4
LIMIT = 12 * 1024 * 1024


def split(values):
    values = np.asarray(values, np.float64)
    high = values.astype(jnp.bfloat16).astype(np.float64)
    low = (values - high).astype(jnp.bfloat16).astype(np.float64)
    return high.astype(np.float32), low.astype(np.float32)


def basis(extent):
    n, half = np.arange(extent), extent // 2
    rows = [np.full(extent, math.sqrt(1.0 / extent)), (1.0 - 2.0 * (n % 2)) * math.sqrt(1.0 / extent)]
    freqs = [0, half]
    for k in range(1, half):
        angle = 2.0 * math.pi * ((k * n) % extent) / extent
        rows += [math.sqrt(2.0 / extent) * np.cos(angle), math.sqrt(2.0 / extent) * np.sin(angle)]
        freqs += [k, k]
    return np.stack(rows), np.array(freqs)


def odd_basis(extent):
    n, rows, freqs = np.arange(extent), [], []
    for k in range(1, extent, 2):
        angle = math.pi * ((k * n) % (2 * extent)) / extent
        rows += [math.sqrt(2.0 / extent) * np.cos(angle), math.sqrt(2.0 / extent) * np.sin(angle)]
        freqs += [k, k]
    return np.stack(rows), np.array(freqs)


def lane_table(matrix):
    size = matrix.shape[0]
    table = np.zeros((2 * LANES, 2 * LANES), np.float32)
    for part in range(2):
        for col, values in enumerate(split(matrix)):
            table[part * LANES:part * LANES + size, col * LANES:col * LANES + size] = values
    return table


def row_table(matrix):
    high, low = split(matrix)
    return np.concatenate([high, high, low], axis=1)


def tables(extent):
    half = extent // 2
    full, freqs = basis(extent)
    even, even_freqs = basis(half)
    odd, odd_freqs = odd_basis(half)
    fold = np.array([[1.0, 1.0], [1.0, -1.0]]) / math.sqrt(2.0)
    square = lambda f: (2.0 * math.pi / extent * np.asarray(f, np.float64)) ** 2
    lanes = np.zeros((half, LANES))
    lanes[:, :extent] = square(2 * even_freqs)[:, None] + square(freqs)[None, :]
    lanes[:, extent:2 * extent] = square(odd_freqs)[:, None] + square(freqs)[None, :]
    kern = 1.0 / (square(np.arange(half + 1))[:, None, None] + lanes[None] + screening)
    return [jnp.asarray(t, F32) for t in (
        lane_table(np.kron(fold, full.T)), row_table(full), row_table(full.T),
        row_table(np.concatenate([even, odd])), row_table(np.concatenate([even.T, odd.T])), kern,
        lane_table(np.kron(fold, full)))]


def place_body(count, variants, *refs):
    sems = refs[2 * count]
    rolled_ref = refs[2 * count - 1]
    targets = [*refs[count:2 * count - 1], rolled_ref.at[0]]
    copies = [pltpu.make_async_copy(refs[i], targets[i], sems.at[i]) for i in range(count)]
    for copy in copies[::-1]:
        copy.start()
    copies[-1].wait()
    for i in range(1, len(variants)):
        for at in range(0, rolled_ref.shape[2], LANES):
            rolled_ref[i, :, at:at + LANES] = pltpu.roll(rolled_ref[0, :, at:at + LANES], variants[i], 1)
    for copy in copies[:-1]:
        copy.wait()


def placed(variants, *arrays):
    arrays = [pltpu.with_memory_space_constraint(a, pltpu.HBM) for a in arrays]
    shapes = [a.shape for a in arrays]
    shapes[-1] = (len(variants), *shapes[-1])
    return pl.pallas_call(
        lambda *refs: place_body(len(arrays), variants, *refs),
        out_shape=[pltpu.VMEM(s, F32) for s in shapes],
        in_specs=[pl.BlockSpec(memory_space=pltpu.HBM)] * len(arrays),
        out_specs=[pl.BlockSpec(memory_space=pltpu.VMEM)] * len(arrays),
        scratch_shapes=[pltpu.SemaphoreType.DMA((len(arrays),))],
        compiler_params=pltpu.CompilerParams(vmem_limit_bytes=LIMIT),
        name="place",
    )(*arrays)


def low_of(x):
    return x - x.astype(jnp.bfloat16).astype(F32)


def rows_apply(table, x):
    return jnp.dot(table, jnp.concatenate([x, low_of(x), x], axis=0), preferred_element_type=F32)


def lanes_apply(x, table):
    both = jnp.dot(jnp.concatenate([x, low_of(x)], axis=1), table, preferred_element_type=F32)
    return both[:, :LANES] + both[:, LANES:]


def beside(a, b):
    return jnp.concatenate([a, b], axis=1)


def pair_body(extent, adds, *refs):
    first_ref, prev_ref, fz_ref, fx_ref, ix_ref, fy_ref, iy_ref, kern_ref, iz_ref = refs[:9]
    if adds:
        w_refs, (more_ref, more_e_ref) = refs[9:12], refs[12:14]
        to_first_ref, to_prev_ref, e_ref, t_ref = refs[14:]
    else:
        to_first_ref, to_prev_ref, e_ref, t_ref = refs[9:]
    half = extent // 2
    pitch = t_ref.shape[0] // half
    tiles = math.lcm(extent, LANES) // LANES
    per = tiles * LANES // extent
    runs = extent // per
    row_stride = tiles * runs
    lane = lax.broadcasted_iota(jnp.int32, (extent, LANES), 1)
    low_half = lax.broadcasted_iota(jnp.int32, (half, 2 * LANES), 1) % LANES < extent
    fx, ix, fy, iy = fx_ref[...], ix_ref[...], fy_ref[...], iy_ref[...]

    def dense(ref, y1, t):
        return ref[pl.ds(tiles * y1 + t, extent, stride=row_stride), :]

    def row(parts, y0):
        t, off = divmod(y0 * extent, LANES)
        if off + extent <= LANES:
            a, b = parts[0][t], parts[1][t]
            inside = lane < off + extent
            if off + 2 * extent > LANES:
                inside &= lane >= off
            return jnp.where(inside, a, b)
        a = jnp.where(lane >= off, parts[0][t], parts[0][t + 1])
        b = jnp.where(lane < extent, parts[1][t], parts[1][t + 1])
        return jnp.where((lane >= off + extent - LANES) & (lane < off), b, a)

    def turned_table(off):
        if off == 0:
            return fz_ref[...]
        cuts = [fz_ref[at + s:at + e] for at in (0, LANES) for s, e in ((LANES - off, LANES), (0, LANES - off))]
        return jnp.concatenate(cuts, axis=0)

    steps = runs // 2
    parts = []
    for y1 in range(steps):
        both = [[dense(first_ref, y1 + h * steps, t) * dense(prev_ref, y1 + h * steps, t)
                 for t in range(tiles)] for h in range(2)]
        parts.append([both[0], [pltpu.roll(p, extent, 1) for p in both[1]]])

    def rows_of(y):
        return pl.ds(y * pitch, extent)

    def along_rows(table):
        for y in range(0, half, 2):
            out = rows_apply(table, beside(t_ref[rows_of(y), :], t_ref[rows_of(y + 1), :]))
            t_ref[rows_of(y), :] = out[:, :LANES]
            t_ref[rows_of(y + 1), :] = out[:, LANES:]

    for y0 in range(per):
        after = lanes_apply(jnp.concatenate([row(parts[y1], y0) for y1 in range(steps)], axis=0),
                            turned_table(y0 * extent % LANES))
        for y1 in range(steps):
            t_ref[rows_of(y1 * per + y0), :] = after[y1 * extent:(y1 + 1) * extent]
    along_rows(fx)

    for p in range(half):
        at = [pl.ds(2 * p + i, half, stride=pitch) for i in range(2)]
        out = rows_apply(fy, beside(t_ref[at[0], :], t_ref[at[1], :]))
        ks = beside(kern_ref[0], kern_ref[half]) if p == 0 else beside(kern_ref[p], kern_ref[p])
        out = rows_apply(iy, jnp.where(low_half, out[:half], out[half:]) * ks)
        out = jnp.where(low_half, out[:half], out[half:])
        t_ref[at[0], :] = out[:, :LANES]
        t_ref[at[1], :] = out[:, LANES:]

    if adds:
        w_own, w_first, w_prev = (w_ref[:1, :] for w_ref in w_refs)
    total = jnp.zeros((extent, LANES), F32)
    turned_lane = (lane + LANES - extent) % LANES
    tile_of = {}

    def finish(t):
        nonlocal total
        for y1 in range(steps):
            for h in range(2):
                v = tile_of.pop((t, y1, h))
                if h:
                    v = pltpu.roll(v, LANES - extent, 1)
                run = y1 + h * steps
                prev, first = dense(prev_ref, run, t), dense(first_ref, run, t)
                at = pl.ds(tiles * run + t, extent, stride=row_stride)
                pv, fv = prev * v, first * v
                to_first_ref[at, :] = w_prev * pv if adds else pv
                to_prev_ref[at, :] = w_first * fv + w_own * more_ref[at, :] if adds else fv
                total = total + first * pv

    along_rows(ix)
    for y0 in range(per):
        start = y0 * extent
        after = lanes_apply(jnp.concatenate([t_ref[rows_of(y1 * per + y0), :] for y1 in range(steps)], axis=0), iz_ref[y0])
        for t in range(start // LANES, (start + extent - 1) // LANES + 1):
            for y1 in range(steps):
                piece = after[y1 * extent:(y1 + 1) * extent]
                for h in range(2):
                    held = tile_of.get((t, y1, h))
                    where = turned_lane if h else lane
                    tile_of[t, y1, h] = piece if held is None else jnp.where(where >= start - t * LANES, piece, held)
        if (start + extent) // LANES > start // LANES:
            finish(start // LANES)
    e_ref[...] = jnp.broadcast_to(jnp.sum(total), e_ref.shape)
    if adds:
        e_ref[...] = w_prev * (w_first * e_ref[...] + w_own * more_e_ref[...])


def pair_call(first, prev, constants, weights, more, count):
    rows = first.shape[0]
    extent = round((rows * LANES) ** (1.0 / 3.0))
    dense = jax.ShapeDtypeStruct((rows, LANES), F32)
    vm = pl.BlockSpec(memory_space=pltpu.VMEM)
    outs = [dense, dense, jax.ShapeDtypeStruct((count, LANES), F32)]
    operands = [first, prev, *constants, *weights, *more]
    return pl.pallas_call(
        lambda *refs: pair_body(extent, 1 if more else 0, *refs),
        out_shape=outs,
        in_specs=[vm] * len(operands),
        out_specs=[vm] * len(outs),
        scratch_shapes=[pltpu.VMEM((extent // 2 * (extent + PAD), LANES), F32)],
        compiler_params=pltpu.CompilerParams(vmem_limit_bytes=LIMIT),
    )(*operands)


def combine_body(scale, e_scale, w_ref, mine_ref, back_ref, behind_ref, everyone_ref, out_ref, e_ref, sum_ref, e_sum_ref, sems):
    count = sems.shape[0] - 1
    size = sum_ref.shape[0] // count
    e_sum_ref[...] = e_scale * jnp.sum(everyone_ref[...], axis=0, keepdims=True)[:, :1]
    copies = [pltpu.make_async_copy(e_sum_ref, e_ref, sems.at[count])]
    copies[0].start()
    for i in range(count):
        at = pl.ds(i * size, size)
        sum_ref[at, :] = scale * (w_ref[:1, :] * mine_ref[at, :] + back_ref[at, :] + behind_ref[at, :])
        copies.append(pltpu.make_async_copy(sum_ref.at[at], out_ref.at[at], sems.at[i]))
        copies[-1].start()
    for copy in copies:
        copy.wait()


AXES = ("blk", "grp")


def moved(value, blocks, groups):
    n_blk, n_grp = lax.axis_size("blk"), lax.axis_size("grp")
    pairs = [(b * n_grp + g, (b + blocks) % n_blk * n_grp + (g + groups) % n_grp)
             for b in range(n_blk) for g in range(n_grp)]
    return lax.ppermute(value, AXES, pairs)


def local(orbitals, occupation):
    count = lax.axis_size(AXES)
    cells = orbitals.size
    weight = jnp.broadcast_to(occupation[:, None], (8, LANES))
    own = orbitals.reshape(cells // LANES, LANES)
    partner = moved(own, 0, 1)
    previous = moved(own, 1, 0)
    w_partner, w_previous = moved(weight, 0, 1), moved(weight, 1, 0)
    extent = round(cells ** (1.0 / 3.0))
    variants = [y0 * extent % LANES for y0 in range(math.lcm(extent, LANES) // extent)]
    mine_own, *constants = placed(variants, own, *tables(extent))
    mine, part, share = pair_call(mine_own, previous, constants, (), (), count)
    to_partner, to_previous, share = pair_call(
        partner, previous, constants, (weight, w_partner, w_previous), (part, share), count)
    back = moved(to_partner, 0, 1)
    behind = moved(to_previous, -1, 0)
    everyone = lax.all_to_all(share, AXES, 0, 0, tiled=True)
    vm = pl.BlockSpec(memory_space=pltpu.VMEM)
    exchange, energy = pl.pallas_call(
        lambda *refs: combine_body(-mixing, -2.0 * mixing / (2.0 * cells * count), *refs),
        out_shape=(jax.ShapeDtypeStruct(own.shape, F32), jax.ShapeDtypeStruct((1, 1), F32)),
        in_specs=[vm] * 5, out_specs=[pl.BlockSpec(memory_space=pltpu.HBM)] * 2,
        scratch_shapes=[pltpu.VMEM(own.shape, F32), pltpu.VMEM((1, 1), F32),
                        pltpu.SemaphoreType.DMA((math.gcd(own.shape[0] // 8, PARTS) + 1,))],
        compiler_params=pltpu.CompilerParams(vmem_limit_bytes=LIMIT),
        name="combine",
    )(w_previous, mine, back, behind, everyone)
    return exchange.reshape(orbitals.shape), energy.reshape(())


def solution(mesh):
    return jax.shard_map(local, mesh=mesh, in_specs=(P(AXES, None), P(AXES)),
                         out_specs=(P(AXES, None), P()), check_vma=False)
```

```python
import math
import numpy as np
import jax
import jax.numpy as jnp
from jax import lax
from jax.sharding import PartitionSpec as P
from jax.experimental import pallas as pl
from jax.experimental.pallas import tpu as pltpu


mixing = 0.25
screening = 0.1
LANES = 128
F32 = jnp.float32
BF16 = jnp.bfloat16
PAD = 8
PARTS = 6
LIMIT = 12 * 1024 * 1024


def split(values):
    values = np.asarray(values, np.float64)
    high = values.astype(jnp.bfloat16).astype(np.float64)
    low = (values - high).astype(jnp.bfloat16).astype(np.float64)
    return high.astype(np.float32), low.astype(np.float32)


def basis(extent):
    n, half = np.arange(extent), extent // 2
    rows = [np.full(extent, math.sqrt(1.0 / extent)), (1.0 - 2.0 * (n % 2)) * math.sqrt(1.0 / extent)]
    freqs = [0, half]
    for k in range(1, half):
        angle = 2.0 * math.pi * ((k * n) % extent) / extent
        rows += [math.sqrt(2.0 / extent) * np.cos(angle), math.sqrt(2.0 / extent) * np.sin(angle)]
        freqs += [k, k]
    return np.stack(rows), np.array(freqs)


def odd_basis(extent):
    n, rows, freqs = np.arange(extent), [], []
    for k in range(1, extent, 2):
        angle = math.pi * ((k * n) % (2 * extent)) / extent
        rows += [math.sqrt(2.0 / extent) * np.cos(angle), math.sqrt(2.0 / extent) * np.sin(angle)]
        freqs += [k, k]
    return np.stack(rows), np.array(freqs)


def lane_table(matrix):
    size = matrix.shape[0]
    table = np.zeros((2 * LANES, 2 * LANES), np.float32)
    for part in range(2):
        for col, values in enumerate(split(matrix)):
            table[part * LANES:part * LANES + size, col * LANES:col * LANES + size] = values
    return table


def row_table(matrix):
    high, low = split(matrix)
    return np.concatenate([high, high, low], axis=1)


def tables(extent):
    half = extent // 2
    full, freqs = basis(extent)
    even, even_freqs = basis(half)
    odd, odd_freqs = odd_basis(half)
    fold = np.array([[1.0, 1.0], [1.0, -1.0]]) / math.sqrt(2.0)
    square = lambda f: (2.0 * math.pi / extent * np.asarray(f, np.float64)) ** 2
    lanes = np.zeros((half, LANES))
    lanes[:, :extent] = square(2 * even_freqs)[:, None] + square(freqs)[None, :]
    lanes[:, extent:2 * extent] = square(odd_freqs)[:, None] + square(freqs)[None, :]
    kern = 1.0 / (square(np.arange(half + 1))[:, None, None] + lanes[None] + screening)
    narrow = [jnp.asarray(t, BF16) for t in (
        lane_table(np.kron(fold, full.T)), row_table(full), row_table(full.T),
        row_table(np.concatenate([even, odd])), row_table(np.concatenate([even.T, odd.T])))]
    return [*narrow, jnp.asarray(kern, F32), jnp.asarray(lane_table(np.kron(fold, full)), F32)]


def place_body(count, variants, *refs):
    plain_ref, sems = refs[2 * count:]
    rolled_ref = refs[2 * count - 1]
    targets = [*refs[count:2 * count - 1], plain_ref]
    copies = [pltpu.make_async_copy(refs[i], targets[i], sems.at[i]) for i in range(count)]
    for copy in copies[::-1]:
        copy.start()
    copies[-1].wait()
    for i, shift in enumerate(variants):
        for at in range(0, plain_ref.shape[1], LANES):
            part = plain_ref[:, at:at + LANES]
            rolled_ref[i, :, at:at + LANES] = (pltpu.roll(part, shift, 1) if shift else part).astype(BF16)
    for copy in copies[:-1]:
        copy.wait()


def placed(variants, *arrays):
    arrays = [pltpu.with_memory_space_constraint(a, pltpu.HBM) for a in arrays]
    last = arrays[-1].shape
    outs = [pltpu.VMEM(a.shape, a.dtype) for a in arrays[:-1]] + [pltpu.VMEM((len(variants), *last), BF16)]
    return pl.pallas_call(
        lambda *refs: place_body(len(arrays), variants, *refs),
        out_shape=outs,
        in_specs=[pl.BlockSpec(memory_space=pltpu.HBM)] * len(arrays),
        out_specs=[pl.BlockSpec(memory_space=pltpu.VMEM)] * len(arrays),
        scratch_shapes=[pltpu.VMEM(last, F32), pltpu.SemaphoreType.DMA((len(arrays),))],
        compiler_params=pltpu.CompilerParams(vmem_limit_bytes=LIMIT),
        name="place",
    )(*arrays)


def low_of(x):
    return x - x.astype(BF16).astype(F32)


def rows_apply(table, x):
    return jnp.dot(table, jnp.concatenate([x, low_of(x), x], axis=0).astype(BF16), preferred_element_type=F32)


def lanes_apply(x, table):
    both = jnp.dot(jnp.concatenate([x, low_of(x)], axis=1).astype(BF16), table, preferred_element_type=F32)
    return both[:, :LANES] + both[:, LANES:]


def beside(a, b):
    return jnp.concatenate([a, b], axis=1)


def pair_body(extent, adds, *refs):
    first_ref, prev_ref, fz_ref, fx_ref, ix_ref, fy_ref, iy_ref, kern_ref, iz_ref = refs[:9]
    if adds:
        w_refs, (more_ref, more_e_ref) = refs[9:12], refs[12:14]
        to_first_ref, to_prev_ref, e_ref, t_ref, mid_ref = refs[14:]
    else:
        to_first_ref, to_prev_ref, e_ref, t_ref, mid_ref = refs[9:]
    half = extent // 2
    pitch = t_ref.shape[0] // half
    tiles = math.lcm(extent, LANES) // LANES
    per = tiles * LANES // extent
    runs = extent // per
    row_stride = tiles * runs
    lane = lax.broadcasted_iota(jnp.int32, (extent, LANES), 1)
    low_half = lax.broadcasted_iota(jnp.int32, (half, 2 * LANES), 1) % LANES < extent
    fx, ix, fy, iy = fx_ref[...], ix_ref[...], fy_ref[...], iy_ref[...]

    def dense(ref, y1, t):
        return ref[pl.ds(tiles * y1 + t, extent, stride=row_stride), :]

    def row(parts, y0):
        t, off = divmod(y0 * extent, LANES)
        if off + extent <= LANES:
            a, b = parts[0][t], parts[1][t]
            inside = lane < off + extent
            if off + 2 * extent > LANES:
                inside &= lane >= off
            return jnp.where(inside, a, b)
        a = jnp.where(lane >= off, parts[0][t], parts[0][t + 1])
        b = jnp.where(lane < extent, parts[1][t], parts[1][t + 1])
        return jnp.where((lane >= off + extent - LANES) & (lane < off), b, a)

    def turned_table(off):
        if off == 0:
            return fz_ref[...]
        cuts = [fz_ref[at + s:at + e] for at in (0, LANES) for s, e in ((LANES - off, LANES), (0, LANES - off))]
        return jnp.concatenate(cuts, axis=0)

    steps = runs // 2
    parts = []
    for y1 in range(steps):
        both = [[dense(first_ref, y1 + h * steps, t) * dense(prev_ref, y1 + h * steps, t)
                 for t in range(tiles)] for h in range(2)]
        parts.append([both[0], [pltpu.roll(p, extent, 1) for p in both[1]]])

    def rows_of(y):
        return pl.ds(y * pitch, extent)

    def along_rows(table):
        for y in range(0, half, 2):
            out = rows_apply(table, beside(t_ref[rows_of(y), :], t_ref[rows_of(y + 1), :]))
            t_ref[rows_of(y), :] = out[:, :LANES]
            t_ref[rows_of(y + 1), :] = out[:, LANES:]

    for y0 in range(per):
        after = lanes_apply(jnp.concatenate([row(parts[y1], y0) for y1 in range(steps)], axis=0),
                            turned_table(y0 * extent % LANES))
        for y1 in range(steps):
            t_ref[rows_of(y1 * per + y0), :] = after[y1 * extent:(y1 + 1) * extent]
    along_rows(fx)

    def column(p):
        return [pl.ds(2 * p + i, half, stride=pitch) for i in range(2)]

    for p in range(half):
        at = column(p)
        out = rows_apply(fy, beside(t_ref[at[0], :], t_ref[at[1], :]))
        ks = beside(kern_ref[0], kern_ref[half]) if p == 0 else beside(kern_ref[p], kern_ref[p])
        out = jnp.where(low_half, out[:half], out[half:]) * ks
        mid_ref[p] = out
    for p in range(half):
        at = column(p)
        out = rows_apply(iy, mid_ref[p])
        out = jnp.where(low_half, out[:half], out[half:])
        t_ref[at[0], :] = out[:, :LANES]
        t_ref[at[1], :] = out[:, LANES:]

    if adds:
        w_own, w_first, w_prev = (w_ref[:1, :] for w_ref in w_refs)
    total = jnp.zeros((extent, LANES), F32)
    turned_lane = (lane + LANES - extent) % LANES
    tile_of = {}

    def finish(t):
        nonlocal total
        for y1 in range(steps):
            for h in range(2):
                v = tile_of.pop((t, y1, h))
                if h:
                    v = pltpu.roll(v, LANES - extent, 1)
                run = y1 + h * steps
                prev, first = dense(prev_ref, run, t), dense(first_ref, run, t)
                at = pl.ds(tiles * run + t, extent, stride=row_stride)
                pv, fv = prev * v, first * v
                to_first_ref[at, :] = w_prev * pv if adds else pv
                to_prev_ref[at, :] = w_first * fv + w_own * more_ref[at, :] if adds else fv
                total = total + first * pv

    along_rows(ix)
    for y0 in range(per):
        start = y0 * extent
        after = lanes_apply(jnp.concatenate([t_ref[rows_of(y1 * per + y0), :] for y1 in range(steps)], axis=0), iz_ref[y0])
        for t in range(start // LANES, (start + extent - 1) // LANES + 1):
            for y1 in range(steps):
                piece = after[y1 * extent:(y1 + 1) * extent]
                for h in range(2):
                    held = tile_of.get((t, y1, h))
                    where = turned_lane if h else lane
                    tile_of[t, y1, h] = piece if held is None else jnp.where(where >= start - t * LANES, piece, held)
        if (start + extent) // LANES > start // LANES:
            finish(start // LANES)
    e_ref[...] = jnp.broadcast_to(jnp.sum(total), e_ref.shape)
    if adds:
        e_ref[...] = w_prev * (w_first * e_ref[...] + w_own * more_e_ref[...])


def pair_call(first, prev, constants, weights, more, count):
    rows = first.shape[0]
    extent = round((rows * LANES) ** (1.0 / 3.0))
    dense = jax.ShapeDtypeStruct((rows, LANES), F32)
    vm = pl.BlockSpec(memory_space=pltpu.VMEM)
    outs = [dense, dense, jax.ShapeDtypeStruct((count, LANES), F32)]
    operands = [first, prev, *constants, *weights, *more]
    return pl.pallas_call(
        lambda *refs: pair_body(extent, 1 if more else 0, *refs),
        out_shape=outs,
        in_specs=[vm] * len(operands),
        out_specs=[vm] * len(outs),
        scratch_shapes=[pltpu.VMEM((extent // 2 * (extent + PAD), LANES), F32),
                        pltpu.VMEM((extent // 2, extent // 2, 2 * LANES), F32)],
        compiler_params=pltpu.CompilerParams(vmem_limit_bytes=LIMIT),
    )(*operands)


def combine_body(scale, e_scale, w_ref, mine_ref, back_ref, behind_ref, everyone_ref, out_ref, e_ref, sum_ref, e_sum_ref, sems):
    count = sems.shape[0] - 1
    size = sum_ref.shape[0] // count
    e_sum_ref[...] = e_scale * jnp.sum(everyone_ref[...], axis=0, keepdims=True)[:, :1]
    copies = [pltpu.make_async_copy(e_sum_ref, e_ref, sems.at[count])]
    copies[0].start()
    for i in range(count):
        at = pl.ds(i * size, size)
        sum_ref[at, :] = scale * (w_ref[:1, :] * mine_ref[at, :] + back_ref[at, :] + behind_ref[at, :])
        copies.append(pltpu.make_async_copy(sum_ref.at[at], out_ref.at[at], sems.at[i]))
        copies[-1].start()
    for copy in copies:
        copy.wait()


AXES = ("blk", "grp")


def moved(value, blocks, groups):
    n_blk, n_grp = lax.axis_size("blk"), lax.axis_size("grp")
    pairs = [(b * n_grp + g, (b + blocks) % n_blk * n_grp + (g + groups) % n_grp)
             for b in range(n_blk) for g in range(n_grp)]
    return lax.ppermute(value, AXES, pairs)


def local(orbitals, occupation):
    count = lax.axis_size(AXES)
    cells = orbitals.size
    weight = jnp.broadcast_to(occupation[:, None], (8, LANES))
    own = orbitals.reshape(cells // LANES, LANES)
    partner = moved(own, 0, 1)
    previous = moved(own, 1, 0)
    w_partner, w_previous = moved(weight, 0, 1), moved(weight, 1, 0)
    extent = round(cells ** (1.0 / 3.0))
    variants = [y0 * extent % LANES for y0 in range(math.lcm(extent, LANES) // extent)]
    mine_own, *constants = placed(variants, own, *tables(extent))
    mine, part, share = pair_call(mine_own, previous, constants, (), (), count)
    to_partner, to_previous, share = pair_call(
        partner, previous, constants, (weight, w_partner, w_previous), (part, share), count)
    back = moved(to_partner, 0, 1)
    behind = moved(to_previous, -1, 0)
    everyone = lax.all_to_all(share, AXES, 0, 0, tiled=True)
    vm = pl.BlockSpec(memory_space=pltpu.VMEM)
    exchange, energy = pl.pallas_call(
        lambda *refs: combine_body(-mixing, -2.0 * mixing / (2.0 * cells * count), *refs),
        out_shape=(jax.ShapeDtypeStruct(own.shape, F32), jax.ShapeDtypeStruct((1, 1), F32)),
        in_specs=[vm] * 5, out_specs=[pl.BlockSpec(memory_space=pltpu.HBM)] * 2,
        scratch_shapes=[pltpu.VMEM(own.shape, F32), pltpu.VMEM((1, 1), F32),
                        pltpu.SemaphoreType.DMA((math.gcd(own.shape[0] // 8, PARTS) + 1,))],
        compiler_params=pltpu.CompilerParams(vmem_limit_bytes=LIMIT),
        name="combine",
    )(w_previous, mine, back, behind, everyone)
    return exchange.reshape(orbitals.shape), energy.reshape(())


def solution(mesh):
    return jax.shard_map(local, mesh=mesh, in_specs=(P(AXES, None), P(AXES)),
                         out_specs=(P(AXES, None), P()), check_vma=False)
```
